32 devices in a mesh: seq: 8 (over z, x), head: 4 (over y, core).
Axes of the slice: x: 2, y: 2, z: 4, core: 2. Of those that a mesh axis runs over, the one named last changes fastest.
Arguments:
- queries: bfloat16 [2048, 64, 128], P('seq', 'head'), may hold values from -360 to 360
- head_weights: bfloat16 [2048, 64], P('seq', 'head'), may hold values from -0.75 to 0.75
- keys: bfloat16 [2048, 128], P('seq'), may hold values from -6 to 6
- targets: bfloat16 [2048, 2048], P('seq'), may hold values from 0.0099487305 to 10
- chosen: int32 [16, 16], P('seq'), may hold values from -1 to 15, as said below
- tile_block: int32 [16], replicated, may hold values from 0 to 15, as said below
Outputs:
- query_grads: bfloat16 [2048, 64, 128], P('seq', 'head')
- weight_grads: float32 [2048, 64], P('seq', 'head')
- key_grads: float32 [2048, 128], P('seq')
- loss: float32 [], replicated
The draws below stay inside these ranges and needn't reach their ends.
Inputs may be any that keep to these rules, and one draw needn't show every extreme that they name: `tile_block`: a permutation of 0 to 15; each aligned group of 4 stored positions holds the global blocks of that same group. `chosen`: slot 0 of stored tile p is tile_block[p]; live entries of a row are distinct, none exceeds tile_block[p], and they precede the -1 entries; over all tiles of one device of seq, at most 1 distinct live block is stored on any one other device.
All inputs are finite; a program needn't handle non-finite values.
Results may differ from the reference program's by a relative error of at most 0.0095.
Values may be sent and summed in bfloat16 or wider, within the bound.
No kernel may reach another device: no remote copies, remote signals or barrier semaphores. Data moves between devices by JAX's collectives and lax.ppermute only.
A program may use at most 128 MiB of HBM per device.

```python
import math
import jax
import jax.numpy as jnp
from jax import lax

HEADS = 64
DH = 128
BLOCK = 128
SLOTS = 16
CAP = 1
TOK_DEV = 256
GROUP = 4
TOKENS = 2048
NB = 16
KEYS = 2048


def selection(key):
    tiles_dev = TOK_DEV // BLOCK
    devices_seq = NB // tiles_dev
    positions = jnp.arange(NB, dtype=jnp.int32)
    group_ids = positions // GROUP
    shuffle = jax.random.randint(jax.random.fold_in(key, 101), (NB,), 0, 4096, dtype=jnp.int32)
    order_score = group_ids * (4096 * NB) + shuffle * NB + positions
    tile_block = jnp.argsort(order_score).astype(jnp.int32)
    home_of = jnp.argsort(tile_block).astype(jnp.int32)
    pick_noise = jax.random.randint(jax.random.fold_in(key, 102), (devices_seq, devices_seq, tiles_dev), 0, 4096, dtype=jnp.int32)
    local_iota = jnp.arange(tiles_dev, dtype=jnp.int32)
    pick_score = pick_noise * tiles_dev + local_iota
    slot_rank = jnp.sum((pick_score[:, :, None, :] > pick_score[:, :, :, None]).astype(jnp.int32), axis=3)
    device_iota = jnp.arange(devices_seq, dtype=jnp.int32)
    in_pool = (slot_rank < CAP) | (device_iota[:, None, None] == device_iota[None, :, None])
    pool_mask = in_pool.reshape(devices_seq, NB)[:, home_of]
    requester = positions // tiles_dev
    candidates = pool_mask[requester] & (positions[None, :] < tile_block[:, None])
    priority_noise = jax.random.randint(jax.random.fold_in(key, 104), (NB, NB), 0, 4096, dtype=jnp.int32)
    priority = jnp.where(candidates, priority_noise * NB + positions[None, :], -1)
    top_vals, top_index = lax.top_k(priority, SLOTS - 1)
    live_slot = top_vals >= 0
    others = jnp.where(live_slot, top_index.astype(jnp.int32), -1)
    chosen = jnp.concatenate([tile_block[:, None], others], axis=1).astype(jnp.int32)
    return (tile_block, chosen)


def draw_tile_block(key, part):
    return selection(key)[0]


def draw_chosen(key, part):
    return selection(key)[1]


def draw_queries(key, part):
    base = jax.random.normal(jax.random.fold_in(key, 11), (TOKENS, HEADS, DH), jnp.float32)
    base = jnp.clip(base, -6.0, 6.0)
    return base.astype(jnp.bfloat16)


def levels(key, shape, pieces, smallest, top_value):
    gain = 1.0
    for dim, parts in pieces:
        steps = jax.random.uniform(jax.random.fold_in(jax.random.fold_in(key, 6), dim), (parts,), jnp.float32, smallest / len(pieces), top_value / len(pieces))
        gain = gain * jnp.repeat(jnp.exp(steps), shape[dim] // parts).reshape((-1,) + (1,) * (len(shape) - 1 - dim))
    return gain


def gaussian(own_key, dims, width, most, pieces=(), held_as=jnp.bfloat16):
    array = jax.random.normal(own_key, dims, jnp.float32) * width
    if len(pieces) > 0:
        array = levels(own_key, dims, pieces, -0.22, 0.18) * array
    return jnp.clip(array, min=-most, max=most).astype(held_as)


def setup_inputs(seed: int = 0) -> dict:
    splits = jax.random.split(jax.random.key(seed), 7)
    return {
        "queries": draw_queries(jax.random.fold_in(splits[6], 71), 0),
        "head_weights": gaussian(splits[1], (TOKENS, HEADS), HEADS ** -0.5, 0.75, ((0, 8), (1, 4))),
        "keys": gaussian(splits[2], (TOKENS, DH), 1.0, 6.0, ((0, 8),)),
        "targets": jnp.clip(jnp.exp(math.log(10.0) - 6.912895 * jax.random.uniform(splits[3], (TOKENS, KEYS), jnp.float32) ** levels(splits[3], (TOKENS, KEYS), ((0, 8),), -0.2, 0.2)), 0.0099487305, 10.0).astype(jnp.bfloat16),
        "chosen": draw_chosen(jax.random.fold_in(splits[6], 71), 0),
        "tile_block": draw_tile_block(jax.random.fold_in(splits[6], 71), 0),
    }


loss_scale = 4194304.0


def reference(queries, head_weights, keys, targets, chosen, tile_block):
    score_scale = DH ** -0.5
    positions = jnp.arange(NB, dtype=jnp.int32)
    home_of = jnp.sum(jnp.where(tile_block[None, :] == positions[:, None], positions[None, :], 0), axis=1).astype(jnp.int32)
    live_slot = chosen >= 0
    position = home_of[jnp.maximum(chosen, 0)]
    key_blocks = keys.reshape(NB, BLOCK, DH)
    fetched = key_blocks[position]
    offsets = jnp.arange(BLOCK, dtype=jnp.int32)
    causal = offsets[None, :] <= offsets[:, None]
    own_slot = chosen == tile_block[:, None]
    live_mask = live_slot[:, None, :, None] & ((~own_slot)[:, None, :, None] | causal[None, :, None, :])
    live_mask = live_mask.reshape(TOKENS, KEYS)
    query_tiles = queries.reshape(NB, BLOCK, HEADS, DH)
    weight_tiles = head_weights.astype(jnp.float32).reshape(NB, BLOCK, HEADS)

    def dot_values(query_tile, key_tile):
        return jnp.einsum('qhd,kd->qhk', query_tile.astype(jnp.float32), key_tile.reshape(-1, DH).astype(jnp.float32), precision=lax.Precision.HIGHEST)

    def forward(operands):
        query_tile, weight_tile, key_tile = operands
        values = dot_values(query_tile, key_tile)
        return score_scale * jnp.sum(jnp.maximum(values, 0.0) * weight_tile[:, :, None], axis=1)

    scores = lax.map(forward, (query_tiles, weight_tiles, fetched)).reshape(TOKENS, KEYS)
    row_max = jnp.max(jnp.where(live_mask, scores, -1e30), axis=1)
    exp_terms = jnp.where(live_mask, jnp.exp(jnp.where(live_mask, scores - row_max[:, None], 0.0)), 0.0)
    row_norm = jnp.sum(exp_terms, axis=1)
    softmax_vals = exp_terms / row_norm[:, None]
    target_vals = jnp.where(live_mask, targets.astype(jnp.float32), 0.0)
    target_prob = target_vals / jnp.sum(target_vals, axis=1)[:, None]
    log_soft = scores - row_max[:, None] - jnp.log(row_norm)[:, None]
    kl_sum = jnp.sum(jnp.where(live_mask, target_prob * (jnp.log(jnp.where(live_mask, target_prob, 1.0)) - log_soft), 0.0))
    pair_count = jnp.sum(live_mask.astype(jnp.float32))
    grad_scores = loss_scale * KEYS * (softmax_vals - target_prob) / pair_count
    grad_tiles = grad_scores.reshape(NB, BLOCK, KEYS)

    def backward(operands):
        query_tile, weight_tile, key_tile, grad_tile = operands
        key_rows = key_tile.reshape(-1, DH)
        values = dot_values(query_tile, key_tile)
        weight_grad = score_scale * jnp.sum(jnp.maximum(values, 0.0) * grad_tile[:, None, :], axis=2)
        dot_grads = (score_scale * weight_tile[:, :, None] * grad_tile[:, None, :] * (values > 0).astype(jnp.float32)).astype(jnp.bfloat16)
        query_grad = jnp.einsum('qhk,kd->qhd', dot_grads.astype(jnp.float32), key_rows.astype(jnp.float32), precision=lax.Precision.HIGHEST).astype(jnp.bfloat16)
        key_grad = jnp.einsum('qhk,qhd->kd', dot_grads.astype(jnp.float32), query_tile.astype(jnp.float32), precision=lax.Precision.HIGHEST)
        return query_grad, weight_grad, key_grad.reshape(SLOTS, BLOCK, DH)

    query_grads, weight_grads, key_parts = lax.map(backward, (query_tiles, weight_tiles, fetched, grad_tiles))
    key_grads = jax.ops.segment_sum(key_parts.reshape(NB * SLOTS, BLOCK, DH), position.reshape(-1), num_segments=NB)
    return (query_grads.reshape(TOKENS, HEADS, DH), weight_grads.reshape(TOKENS, HEADS), key_grads.reshape(TOKENS, DH), KEYS * kl_sum / pair_count)
```

```python
import functools

import jax
import jax.numpy as jnp
from jax import lax
from jax.experimental import pallas as pl
from jax.experimental.pallas import tpu as pltpu
from jax.sharding import PartitionSpec as P

BLOCK = 128
CAP = 1
LANES = 128
CHUNK = 8
EXTRA = 8
LOSS_SCALE = 4194304.0
bf16, f32, i32 = jnp.bfloat16, jnp.float32, jnp.int32
ANY = pl.BlockSpec(memory_space=pl.ANY)
SMEM = pl.BlockSpec(memory_space=pltpu.SMEM)
VMEM = pl.BlockSpec(memory_space=pltpu.VMEM)
PARAMS = pltpu.CompilerParams(vmem_limit_bytes=60 * 1024 * 1024)


def put_pieces(ref, x):
    for i in range(1, 4):
        piece = x.astype(bf16).astype(f32)
        ref[i : i + 1, :] = piece
        x = x - piece


def sum_pieces(rows):
    return rows[1:2] + rows[2:3] + rows[3:4]


def diagonal(shape):
    return lax.broadcasted_iota(i32, shape, 2) == lax.broadcasted_iota(i32, shape, 1)


def main_kernel(dims, *refs):
    owners, tiles, heads, members, rows, slots, blocks, key_count, shifted = dims
    refs = list(refs)
    chosen_ref, tile_ref, mine_ref = refs[:3]
    other_refs, refs = refs[3 : 2 + members], refs[2 + members :]
    n_keys = owners if shifted else 1
    key_refs, refs = refs[:n_keys], refs[n_keys:]
    target_ref, refs = refs[0], refs[1:]
    ret_refs, refs = refs[:members], refs[members:]
    payload_ref, own_ref, refs = refs[0], refs[1], refs[2:]
    home, q_all, w_all, key_all, key_buf, target_buf, dots_buf, score_buf, wb_buf, wq_buf, dk_buf, info_buf = refs[:12]
    in_sem, key_sem, target_sem = refs[12:]
    me, part = lax.axis_index("seq"), lax.axis_index("head")
    width = q_all.shape[-1]
    step_rows = CHUNK * heads
    steps = rows // CHUNK
    cut = [slice(k * BLOCK, (k + 1) * BLOCK) for k in range(slots)]

    copies = []
    for m in range(members):
        src = mine_ref.at[pl.ds(part * steps, steps)] if m == 0 else other_refs[m - 1]
        copies.append(pltpu.make_async_copy(src.at[:, pl.ds(0, step_rows)], q_all.at[:, m], in_sem.at[2 * m]))
        copies.append(pltpu.make_async_copy(src.at[:, pl.ds(step_rows, CHUNK)], w_all.at[:, m], in_sem.at[2 * m + 1]))
    if shifted:
        key_copies = [pltpu.make_async_copy(r, key_all.at[k], key_sem.at[k]) for k, r in enumerate(key_refs)]
    else:
        key_copies = [pltpu.make_async_copy(key_refs[0], key_all, key_sem.at[0])]
    target_copy = pltpu.make_async_copy(
        target_ref.at[pl.ds(part * rows, rows), pl.ds(0, slots * BLOCK)], target_buf, target_sem.at[0]
    )
    for c in copies + key_copies + [target_copy]:
        c.start()

    def put(p, carry):
        home[tile_ref[p]] = p
        return carry

    lax.fori_loop(0, blocks, put, 0)
    tile = (part * rows) // BLOCK
    first_row = lax.rem(part * rows, BLOCK)
    own_block = tile_ref[me * tiles + tile]
    live, own, owner, local = [], [], [], []
    for k in range(slots):
        c = chosen_ref[tile, k]
        at = home[jnp.maximum(c, 0)]
        live.append((c >= 0).astype(i32))
        own.append((c == own_block).astype(i32))
        owner.append(at // tiles)
        local.append(lax.rem(at, tiles))

    for c in copies:
        c.wait()

    def spread(i, carry):
        for m in range(members):
            w = jnp.broadcast_to(w_all[i, m].astype(f32)[:, None, :], (CHUNK, heads, LANES))
            w = jnp.sum(jnp.where(diagonal(w.shape), w, 0.0), axis=2, keepdims=True)
            w = jnp.broadcast_to(w, (CHUNK, heads, LANES)).reshape(step_rows, LANES)
            wb_buf[i, m] = w
            wq_buf[i, m] = (w * q_all[i, m].astype(f32)).astype(bf16)
        return carry

    lax.fori_loop(0, steps, spread, 0)

    for c in key_copies:
        c.wait()
    for k in range(slots):
        index = lax.rem(me - owner[k] + owners, owners) if shifted else owner[k]
        key_buf[cut[k], :] = key_all[index, pl.ds(pl.multiple_of(local[k] * BLOCK, BLOCK), BLOCK), :]
    counts = jnp.sum(key_all[:, tiles * BLOCK : tiles * BLOCK + EXTRA, :].astype(f32), axis=0)
    n_live = jnp.sum(counts, axis=0, keepdims=True)
    pair_count = (n_live - blocks) * (BLOCK * BLOCK) + blocks * (BLOCK * (BLOCK + 1) // 2)
    score_scale = width ** (-0.5)

    def forward(i, carry):
        q = q_all[i].reshape(members * step_rows, width)
        wb = wb_buf[i].reshape(members * step_rows, LANES)
        at = pl.ds(pl.multiple_of(i * CHUNK, CHUNK), CHUNK)
        for k0 in range(0, slots, 2):
            n = min(2, slots - k0)
            both = slice(k0 * BLOCK, (k0 + n) * BLOCK)
            dots = lax.dot_general(q, key_buf[both, :], (((1,), (1,)), ((), ())), preferred_element_type=f32)
            dots_buf[i, :, both] = dots.astype(bf16)
            for k in range(n):
                terms = jnp.maximum(dots[:, cut[k]], 0.0) * wb
                total = terms[:step_rows]
                for m in range(1, members):
                    total = total + terms[m * step_rows : (m + 1) * step_rows]
                score_buf[at, cut[k0 + k]] = score_scale * jnp.sum(total.reshape(CHUNK, heads, BLOCK), axis=1)
        return carry

    lax.fori_loop(0, steps, forward, 0)

    target_copy.wait()
    row = lax.broadcasted_iota(i32, (rows, BLOCK), 0) + first_row
    col = lax.broadcasted_iota(i32, (rows, BLOCK), 1)
    masks = [col < live[k] * (own[k] * (row + 1) + (1 - own[k]) * BLOCK) for k in range(slots)]
    top = jnp.full((rows, BLOCK), -1e30, f32)
    target_sum = jnp.zeros((rows, BLOCK), f32)
    for k in range(slots):
        top = jnp.maximum(top, jnp.where(masks[k], score_buf[:, cut[k]], -1e30))
        target_sum = target_sum + jnp.where(masks[k], target_buf[:, cut[k]].astype(f32), 0.0)
    row_max = jnp.max(top, axis=1, keepdims=True)
    inverse_target = 1.0 / jnp.sum(target_sum, axis=1, keepdims=True)
    exp_sum = jnp.zeros((rows, BLOCK), f32)
    kl = jnp.zeros((rows, BLOCK), f32)
    for k in range(slots):
        score = jnp.where(masks[k], score_buf[:, cut[k]] - row_max, 0.0)
        exp_sum = exp_sum + jnp.where(masks[k], jnp.exp(score), 0.0)
        prob = jnp.where(masks[k], target_buf[:, cut[k]].astype(f32) * inverse_target, 1.0)
        kl = kl + jnp.where(masks[k], prob * (jnp.log(prob) - score), 0.0)
    row_norm = jnp.sum(exp_sum, axis=1, keepdims=True)
    inverse_norm = 1.0 / row_norm
    kl_rows = jnp.sum(kl, axis=1, keepdims=True) + jnp.log(row_norm)
    loss = key_count * jnp.sum(kl_rows, axis=0, keepdims=True) / pair_count
    factor = score_scale * LOSS_SCALE * key_count / pair_count
    for k in range(slots):
        score = jnp.where(masks[k], score_buf[:, cut[k]] - row_max, 0.0)
        soft = jnp.exp(score) * inverse_norm
        prob = target_buf[:, cut[k]].astype(f32) * inverse_target
        score_buf[:, cut[k]] = jnp.where(masks[k], (soft - prob) * factor, 0.0)

    dk_buf[...] = jnp.zeros_like(dk_buf)

    def backward(i, carry):
        at = pl.ds(pl.multiple_of(i * CHUNK, CHUNK), CHUNK)
        for k in range(slots):
            g = jnp.broadcast_to(score_buf[at, cut[k]][:, None, :], (CHUNK, heads, BLOCK))
            g = g.reshape(step_rows, BLOCK).astype(bf16)
            for m in range(members):
                span = slice(m * step_rows, (m + 1) * step_rows)
                d = dots_buf[i, span, cut[k]]
                dots_buf[i, span, cut[k]] = jnp.where(d > 0, g, jnp.zeros_like(g))
        masked = dots_buf[i]
        summed = jnp.dot(masked, key_buf[...], preferred_element_type=f32)
        wq = wq_buf[i].reshape(members * step_rows, width)
        dk_buf[...] += lax.dot_general(masked, wq, (((0,), (0,)), ((), ())), preferred_element_type=f32)
        for m in range(members):
            r = summed[m * step_rows : (m + 1) * step_rows]
            ret_refs[m][i, :step_rows, :] = (r * wb_buf[i, m]).astype(bf16)
            dot = (r * q_all[i, m].astype(f32)).reshape(CHUNK, heads, width)
            dot = jnp.broadcast_to(jnp.sum(dot, axis=2, keepdims=True), (CHUNK, heads, LANES))
            grad = jnp.sum(jnp.where(diagonal(dot.shape), dot, 0.0), axis=1)
            rest = pltpu.roll(grad - grad.astype(bf16).astype(f32), heads, 1)
            spot = lax.broadcasted_iota(i32, grad.shape, 1)
            ret_refs[m][i, step_rows:, :] = jnp.where(spot < heads, grad, rest).astype(bf16)
        return carry

    lax.fori_loop(0, steps, backward, 0)

    payload_ref[...] = jnp.zeros_like(payload_ref)
    own_ref[...] = jnp.zeros_like(own_ref)
    info_buf[...] = jnp.zeros_like(info_buf)
    put_pieces(info_buf, loss)
    info = info_buf[...].astype(bf16)
    for o in range(owners):
        payload_ref[o, BLOCK:, :] = info
    first = lax.broadcasted_iota(i32, (EXTRA, LANES), 0) == 0
    for k in range(slots):

        @pl.when((live[k] == 1) & (owner[k] != me))
        def _():
            payload_ref[owner[k], :BLOCK, :] = dk_buf[cut[k], :].astype(bf16)
            slot = jnp.full((EXTRA, LANES), local[k]).astype(f32)
            payload_ref[owner[k], BLOCK:, :] = jnp.where(first, slot, info_buf[...]).astype(bf16)

        @pl.when((live[k] == 1) & (owner[k] == me))
        def _():
            own_ref[local[k]] = dk_buf[cut[k], :]


def gather_kernel(owners, tiles, recv_ref, own_ref, out_ref, info_buf):
    totals = [own_ref[l] for l in range(tiles)]
    loss = jnp.zeros((1, LANES), f32)
    for o in range(owners):
        info = recv_ref[o, BLOCK:, :].astype(f32)
        block = recv_ref[o, :BLOCK, :].astype(f32)
        loss = loss + sum_pieces(info)
        for l in range(tiles):
            totals[l] = totals[l] + jnp.where(info[0:1] == l, block, 0.0)
    for l in range(tiles):
        out_ref[l * BLOCK : (l + 1) * BLOCK, :] = totals[l].astype(bf16)
    info_buf[...] = jnp.zeros_like(info_buf)
    put_pieces(info_buf, loss)
    out_ref[tiles * BLOCK :, :] = info_buf[...].astype(bf16)


def add_kernel(size, a_ref, b_ref, out_ref, info_buf):
    out_ref[:size, :] = (a_ref[:size, :].astype(f32) + b_ref[:size, :].astype(f32)).astype(bf16)
    loss = sum_pieces(a_ref[size:, :].astype(f32)) + sum_pieces(b_ref[size:, :].astype(f32))
    info_buf[...] = jnp.zeros_like(info_buf)
    put_pieces(info_buf, loss)
    out_ref[size:, :] = info_buf[...].astype(bf16)


def last_kernel(size, a_ref, b_ref, out_ref, loss_ref):
    out_ref[...] = a_ref[:size, :].astype(f32) + b_ref[:size, :].astype(f32)
    loss = sum_pieces(a_ref[size:, :].astype(f32)) + sum_pieces(b_ref[size:, :].astype(f32))
    loss_ref[0] = loss[0, 0]


def place_kernel(heads, members, *refs):
    parts, (grad_ref, weight_ref) = refs[:members], refs[members:]
    steps = parts[0].shape[0]
    step_rows = CHUNK * heads
    part = lax.axis_index("head")
    for m in range(members):
        piece = part ^ m
        grad_ref[pl.ds(piece * steps, steps)] = parts[m][:, :step_rows, :]
        x = parts[m][:, step_rows:, :].astype(f32).reshape(steps * CHUNK, LANES)
        at = pl.multiple_of(piece * (steps * CHUNK), CHUNK)
        weight_ref[pl.ds(at, steps * CHUNK), :] = x[:, :heads] + x[:, heads : 2 * heads]


def local(sizes, queries, head_weights, keys, targets, chosen, tile_block):
    owners, members = sizes
    row_count, heads, width = queries.shape
    tiles = row_count // BLOCK
    rows = row_count // members
    blocks = tile_block.shape[0]
    slots = min(chosen.shape[1], tiles + (owners - 1) * CAP)
    key_count = targets.shape[1]
    steps = rows // CHUNK
    step_rows = CHUNK * heads
    shifted = owners <= 8
    part = lax.axis_index("head")

    mine = jnp.concatenate(
        [
            queries.reshape(members * steps, step_rows, width),
            jnp.pad(head_weights, ((0, 0), (0, LANES - heads))).reshape(members * steps, CHUNK, LANES),
        ],
        axis=1,
    )
    others = []
    for k in range(1, members):
        piece = lax.dynamic_slice_in_dim(mine, (part ^ k) * steps, steps, axis=0)
        others.append(lax.ppermute(piece, "head", [(i, i ^ k) for i in range(members)]))
    n_live = jnp.sum((chosen >= 0).astype(bf16), axis=1)
    extra = jnp.pad(jnp.broadcast_to(n_live[:, None], (tiles, LANES)), ((0, EXTRA - tiles), (0, 0)))
    key_payload = jnp.concatenate([keys, extra], axis=0)
    if shifted:
        tables = [key_payload]
        for k in range(1, owners):
            tables.append(lax.ppermute(key_payload, "seq", [(i, (i + k) % owners) for i in range(owners)]))
    else:
        tables = [lax.all_gather(key_payload, "seq")]

    dims = (owners, tiles, heads, members, rows, slots, blocks, key_count, shifted)
    results = pl.pallas_call(
        functools.partial(main_kernel, dims),
        in_specs=[SMEM, SMEM] + [ANY] * (members + len(tables) + 1),
        out_specs=[VMEM] * (members + 2),
        out_shape=[jax.ShapeDtypeStruct((steps, step_rows + CHUNK, width), bf16)] * members
        + [
            jax.ShapeDtypeStruct((owners, BLOCK + EXTRA, width), bf16),
            jax.ShapeDtypeStruct((tiles, BLOCK, width), f32),
        ],
        scratch_shapes=[
            pltpu.SMEM((blocks,), i32),
            pltpu.VMEM((steps, members, step_rows, width), bf16),
            pltpu.VMEM((steps, members, CHUNK, LANES), bf16),
            pltpu.VMEM((owners, tiles * BLOCK + EXTRA, width), bf16),
            pltpu.VMEM((slots * BLOCK, width), bf16),
            pltpu.VMEM((rows, slots * BLOCK), bf16),
            pltpu.VMEM((steps, members * step_rows, slots * BLOCK), bf16),
            pltpu.VMEM((rows, slots * BLOCK), f32),
            pltpu.VMEM((steps, members, step_rows, LANES), f32),
            pltpu.VMEM((steps, members, step_rows, width), bf16),
            pltpu.VMEM((slots * BLOCK, width), f32),
            pltpu.VMEM((EXTRA, LANES), f32),
            pltpu.SemaphoreType.DMA((2 * members,)),
            pltpu.SemaphoreType.DMA((owners,)),
            pltpu.SemaphoreType.DMA((1,)),
        ],
        compiler_params=PARAMS,
        name="main",
    )(chosen, tile_block, mine, *others, *tables, targets)
    parts, payload, own = results[:members], results[members], results[members + 1]

    arrived = lax.all_to_all(payload, "seq", split_axis=0, concat_axis=0, tiled=True)
    back = [parts[0]]
    for k in range(1, members):
        back.append(lax.ppermute(parts[k], "head", [(i, i ^ k) for i in range(members)]))

    size = tiles * BLOCK
    summed = jax.ShapeDtypeStruct((size + EXTRA, width), bf16)
    info = [pltpu.VMEM((EXTRA, LANES), f32)]
    total = pl.pallas_call(
        functools.partial(gather_kernel, owners, tiles), out_shape=summed, scratch_shapes=info, name="gather"
    )(arrived, own)
    step = 1
    while 2 * step < members:
        pair = lax.ppermute(total, "head", [(i, i ^ step) for i in range(members)])
        total = pl.pallas_call(functools.partial(add_kernel, size), out_shape=summed, scratch_shapes=info, name="add")(total, pair)
        step *= 2
    pair = lax.ppermute(total, "head", [(i, i ^ step) for i in range(members)])
    key_grads, loss = pl.pallas_call(
        functools.partial(last_kernel, size),
        out_specs=[VMEM, SMEM],
        out_shape=[jax.ShapeDtypeStruct((size, width), f32), jax.ShapeDtypeStruct((1,), f32)],
        name="last",
    )(total, pair)
    query_grads, weight_grads = pl.pallas_call(
        functools.partial(place_kernel, heads, members),
        out_shape=[
            jax.ShapeDtypeStruct((members * steps, step_rows, width), bf16),
            jax.ShapeDtypeStruct((row_count, heads), f32),
        ],
        name="place",
    )(*back)
    return query_grads.reshape(row_count, heads, width), weight_grads, key_grads, loss.reshape(())


def solution(mesh):
    placed = (
        P("seq", "head", None),
        P("seq", "head"),
        P("seq", None),
        P("seq", None),
        P("seq", None),
        P(),
    )
    return jax.shard_map(
        functools.partial(local, (mesh.shape["seq"], mesh.shape["head"])),
        mesh=mesh,
        in_specs=placed,
        out_specs=(P("seq", "head", None), P("seq", "head"), P("seq", None), P()),
        check_vma=False,
    )
```
